8 devices in a mesh: dp: 1 (over z), tp: 2 (over y), ep: 4 (over x, core).
Axes of the slice: x: 2, y: 2, z: 1, core: 2. Of those that a mesh axis runs over, the one named last changes fastest.
Arguments:
- x_in: bfloat16 [4096, 1024], P(('dp', 'ep', 'tp'))
- norm_gain: bfloat16 [1024], replicated
- w_router: bfloat16 [1024, 32], replicated
- expert_idx: int32 [4096, 8], P(('dp', 'ep', 'tp'))
- w_gate: bfloat16 [32, 1024, 512], P('ep', None, 'tp')
- w_up: bfloat16 [32, 1024, 512], P('ep', None, 'tp')
- w_down: bfloat16 [32, 512, 1024], P('ep', 'tp')
- out_bias: bfloat16 [1024], replicated
- dy_out: bfloat16 [4096, 1024], P(('dp', 'ep', 'tp'))
Outputs:
- output 1: bfloat16 [4096, 1024], P(('dp', 'ep', 'tp'))
- output 2: bfloat16 [4096, 1024], P(('dp', 'ep', 'tp'))
- output 3: float32 [1024], P('dp')
- output 4: float32 [1024, 32], P('dp')
- output 5: float32 [32, 1024, 512], P(('dp', 'ep'), None, 'tp')
- output 6: float32 [32, 1024, 512], P(('dp', 'ep'), None, 'tp')
- output 7: float32 [32, 512, 1024], P(('dp', 'ep'), 'tp')
- output 8: float32 [1024], P('dp')
All inputs are finite; a program needn't handle non-finite values.
Results may differ from the reference program's by a relative error of at most 0.0127574.
Values are sent between devices in bfloat16 or wider.
A program may use at most 1 GiB of HBM per device.

```python
import jax
import jax.numpy as jnp
from jax import lax

TOK = 512
D = 1024
FF = 512
EXPERTS = 32
TOP = 8
EP_DEVS = 4
TP_DEVS = 2
CAP = 256
EPS = 1e-6


def permute_tokens(perm_key):
    return jax.random.permutation(perm_key, TOK)


def draw_routing(route_key):
    n_src = EP_DEVS * TP_DEVS
    key_heavy, key_weight, key_perm = jax.random.split(route_key, 3)
    expert_row = jnp.arange(EXPERTS)[None, :]
    heavy = jax.random.randint(key_heavy, (n_src, 1), 0, EXPERTS)
    is_heavy = expert_row == heavy
    weights = jnp.where(is_heavy, 0, jax.random.randint(key_weight, (n_src, EXPERTS), 2, 5))
    rest = TOK * TOP - CAP
    share = rest * weights // jnp.sum(weights, axis=1, keepdims=True)
    left_over = rest - jnp.sum(share, axis=1, keepdims=True)
    light_rank = jnp.cumsum(jnp.where(is_heavy, 0, 1), axis=1) - 1
    extra = jnp.where(jnp.logical_and(jnp.logical_not(is_heavy), light_rank < left_over), 1, 0)
    counts = jnp.where(is_heavy, CAP, share + extra)
    ends = jnp.cumsum(counts, axis=1)
    position = jnp.arange(TOP)[None, :] * TOK + jnp.arange(TOK)[:, None]
    choice = jnp.sum((position[None, :, :, None] >= ends[:, None, None, :]).astype(jnp.int32), axis=-1)
    perms = jax.vmap(permute_tokens)(jax.random.split(key_perm, n_src))
    choice = jnp.take_along_axis(choice, perms[:, :, None], axis=1)
    return choice.reshape(n_src * TOK, TOP).astype(jnp.int32)


def setup_inputs(seed: int = 0, part: int = 0) -> dict:
    part_key = jax.random.fold_in(jax.random.key(seed), part)
    key_x, key_dy, key_route = jax.random.split(part_key, 3)
    key_g, key_r, key_wg, key_wu, key_wd, key_b = jax.random.split(jax.random.key(seed + 1), 6)
    n_rows = EP_DEVS * TP_DEVS * TOK
    x_in = jax.random.normal(key_x, (n_rows, D), jnp.float32).astype(jnp.bfloat16)
    norm_gain = (1.0 + 0.3 * jax.random.normal(key_g, (D,), jnp.float32)).astype(jnp.bfloat16)
    w_router = (2.0 * D ** -0.5 * jax.random.normal(key_r, (D, EXPERTS), jnp.float32)).astype(jnp.bfloat16)
    w_gate = (D ** -0.5 * jax.random.normal(key_wg, (EXPERTS, D, FF), jnp.float32)).astype(jnp.bfloat16)
    w_up = (D ** -0.5 * jax.random.normal(key_wu, (EXPERTS, D, FF), jnp.float32)).astype(jnp.bfloat16)
    w_down = (1.5 * FF ** -0.5 * jax.random.normal(key_wd, (EXPERTS, FF, D), jnp.float32)).astype(jnp.bfloat16)
    out_bias = (0.5 * jax.random.normal(key_b, (D,), jnp.float32)).astype(jnp.bfloat16)
    dy_out = jax.random.normal(key_dy, (n_rows, D), jnp.float32).astype(jnp.bfloat16)
    expert_idx = draw_routing(key_route)
    return {"x_in": x_in, "norm_gain": norm_gain, "w_router": w_router, "expert_idx": expert_idx, "w_gate": w_gate, "w_up": w_up, "w_down": w_down, "out_bias": out_bias, "dy_out": dy_out}


def to_bf16(values):
    return values + lax.stop_gradient(values.astype(jnp.bfloat16).astype(jnp.float32) - values)


def reference(x_in, norm_gain, w_router, expert_idx, w_gate, w_up, w_down, out_bias, dy_out):
    n_rows = x_in.shape[0]
    rows_max = EP_DEVS * TP_DEVS * CAP
    flat_ids = expert_idx.reshape(-1)
    order = jnp.argsort(flat_ids, stable=True)
    counts = jnp.sum((flat_ids[:, None] == jnp.arange(EXPERTS)[None, :]).astype(jnp.int32), axis=0)
    starts = jnp.cumsum(counts) - counts
    slot_rank = jnp.arange(rows_max)[None, :]
    slot_tok = order[jnp.minimum(starts[:, None] + slot_rank, n_rows * TOP - 1)] // TOP
    slot_ok = slot_rank < counts[:, None]
    copy_pos = (flat_ids * rows_max + jnp.argsort(order) - starts[flat_ids]).reshape(n_rows, TOP)

    def forward(x_f32, gain, router, gate_w, up_w, down_w, bias):
        inv_rms = lax.rsqrt(jnp.mean(x_f32 * x_f32, axis=-1, keepdims=True) + EPS)
        hidden = to_bf16(x_f32 * inv_rms * gain)
        logits = jnp.dot(hidden, router, preferred_element_type=jnp.float32)
        gates = jax.nn.softmax(jnp.take_along_axis(logits, expert_idx, axis=1), axis=-1)

        def one_expert(operands):
            gate_e, up_e, down_e, tok_e, ok_e = operands
            rows_in = jnp.where(ok_e[:, None], hidden[tok_e], 0.0)
            gate_pre = jnp.dot(rows_in, gate_e, preferred_element_type=jnp.float32)
            up_pre = jnp.dot(rows_in, up_e, preferred_element_type=jnp.float32)
            hidden_act = to_bf16(jax.nn.silu(gate_pre) * up_pre)
            return to_bf16(jnp.dot(hidden_act, down_e, preferred_element_type=jnp.float32))

        y_slots = lax.map(jax.checkpoint(one_expert), (gate_w, up_w, down_w, slot_tok, slot_ok))
        y_copy = y_slots.reshape(EXPERTS * rows_max, D)[copy_pos]
        return x_f32 + jnp.sum(gates[:, :, None] * y_copy, axis=1) + bias

    y_f32, pullback = jax.vjp(forward, x_in.astype(jnp.float32), norm_gain.astype(jnp.float32), w_router.astype(jnp.float32), w_gate.astype(jnp.float32), w_up.astype(jnp.float32), w_down.astype(jnp.float32), out_bias.astype(jnp.float32))
    cotangents = pullback(dy_out.astype(jnp.float32))
    return (y_f32.astype(jnp.bfloat16), cotangents[0].astype(jnp.bfloat16), cotangents[1], cotangents[2], cotangents[3], cotangents[4], cotangents[5], cotangents[6])
```

```python
import functools

import jax
import jax.numpy as jnp
from jax import lax
from jax.experimental import pallas as pl
from jax.experimental.pallas import tpu as pltpu
from jax.sharding import PartitionSpec as P

EPS = 1e-6
F32 = jnp.float32
BF16 = jnp.bfloat16


def dot_nn(a, b):
    return jnp.dot(a, b, preferred_element_type=F32)


def dot_nt(a, b):
    return lax.dot_general(a, b, (((1,), (1,)), ((), ())), preferred_element_type=F32)


def dot_tn(a, b):
    return lax.dot_general(a, b, (((0,), (0,)), ((), ())), preferred_element_type=F32)


def expert_step(e, first, h_ref, ht_ref, dy_ref, g_ref, wgu, wd, dwgu, dwd, out_acc, dh_acc, dg_acc):
    half = wd.shape[1]
    rows = h_ref.shape[0]
    lane = lax.broadcasted_iota(jnp.int32, (rows, 128), 1)
    gate = jnp.sum(jnp.where(lane == e, g_ref[...], 0.0), axis=1, keepdims=True)
    on = gate > 0.0
    au = dot_nn(h_ref[...], wgu[e])
    raw = dot_nt(dy_ref[...], wd[e])
    a = au[:, :half]
    u = au[:, half:]
    sig = jax.nn.sigmoid(a)
    silu = a * sig
    act = jnp.where(on, silu * u, 0.0).astype(BF16)
    dg = jnp.sum(jnp.where(on, act.astype(F32) * raw, 0.0), axis=1, keepdims=True)
    dg_acc[...] = jnp.where(lane == e, dg, dg_acc[...])
    d_act = gate * raw
    da = jnp.where(on, d_act * u * sig * (1.0 + a * (1.0 - sig)), 0.0).astype(BF16)
    du = jnp.where(on, d_act * silu, 0.0).astype(BF16)
    dau = jnp.concatenate([da, du], axis=1)
    out_acc[...] += gate * dot_nn(act, wd[e])
    dh_acc[...] += dot_nt(dau, wgu[e])
    dwgu[e] += dot_nn(ht_ref[...], dau)
    gdy = (gate * dy_ref[...].astype(F32)).astype(BF16)
    dwd[e] += dot_tn(act, gdy)


def dense_kernel(h_hbm, dy_hbm, g_hbm, wg_hbm, wu_hbm, wd_hbm, tok_hbm, dg_hbm, dwg_hbm, dwu_hbm, dwd_hbm,
                 h_s, dy_s, g_s, ht_s, wgu, wd, dwgu, dwd, out_acc, dh_acc, dg_acc, tok_s, dg_s,
                 in_sem, w_sem, out_sem, dw_sem):
    n_blk, rows, d = h_hbm.shape
    n_loc, _, half = wg_hbm.shape

    def loads(c, slot):
        return [pltpu.make_async_copy(h_hbm.at[c], h_s.at[slot], in_sem.at[slot, 0]),
                pltpu.make_async_copy(dy_hbm.at[c], dy_s.at[slot], in_sem.at[slot, 1]),
                pltpu.make_async_copy(g_hbm.at[c], g_s.at[slot], in_sem.at[slot, 2])]

    def w_loads(e):
        return [pltpu.make_async_copy(wg_hbm.at[e], wgu.at[e, :, pl.ds(0, half)], w_sem.at[e, 0]),
                pltpu.make_async_copy(wu_hbm.at[e], wgu.at[e, :, pl.ds(half, half)], w_sem.at[e, 1]),
                pltpu.make_async_copy(wd_hbm.at[e], wd.at[e], w_sem.at[e, 2])]

    def dw_stores(e):
        return [pltpu.make_async_copy(dwgu.at[e, :, pl.ds(0, half)], dwg_hbm.at[e], dw_sem.at[e, 0]),
                pltpu.make_async_copy(dwgu.at[e, :, pl.ds(half, half)], dwu_hbm.at[e], dw_sem.at[e, 1]),
                pltpu.make_async_copy(dwd.at[e], dwd_hbm.at[e], dw_sem.at[e, 2])]

    def out_stores(c):
        return [pltpu.make_async_copy(tok_s, tok_hbm.at[c], out_sem.at[0]),
                pltpu.make_async_copy(dg_s, dg_hbm.at[c], out_sem.at[1])]

    for cp in loads(0, 0):
        cp.start()

    def start_w(e, _):
        for cp in w_loads(e):
            cp.start()
        return 0
    lax.fori_loop(0, n_loc, start_w, 0)

    def block(c, _):
        slot = lax.rem(c, 2)
        for cp in loads(c, slot):
            cp.wait()

        @pl.when(c + 1 < n_blk)
        def _():
            for cp in loads(c + 1, 1 - slot):
                cp.start()
        h_ref, dy_ref, g_ref = h_s.at[slot], dy_s.at[slot], g_s.at[slot]
        ht_s[...] = h_ref[...].T
        out_acc[...] = jnp.zeros_like(out_acc)
        dh_acc[...] = jnp.zeros_like(dh_acc)
        dg_acc[...] = jnp.zeros_like(dg_acc)

        def expert(e, _):
            @pl.when(c == 0)
            def _():
                for cp in w_loads(e):
                    cp.wait()
                dwgu[e] = jnp.zeros(dwgu.shape[1:], F32)
                dwd[e] = jnp.zeros(dwd.shape[1:], F32)
            expert_step(e, None, h_ref, ht_s, dy_ref, g_ref, wgu, wd, dwgu, dwd, out_acc, dh_acc, dg_acc)

            @pl.when(c == n_blk - 1)
            def _():
                for cp in dw_stores(e):
                    cp.start()
            return 0
        lax.fori_loop(0, n_loc, expert, 0)

        @pl.when(c > 0)
        def _():
            for cp in out_stores(c - 1):
                cp.wait()
        tok_s[:, pl.ds(0, d)] = out_acc[...].astype(BF16)
        tok_s[:, pl.ds(d, d)] = dh_acc[...].astype(BF16)
        dg_s[...] = dg_acc[...]
        for cp in out_stores(c):
            cp.start()
        return 0
    lax.fori_loop(0, n_blk, block, 0)
    for cp in out_stores(n_blk - 1):
        cp.wait()

    def end_w(e, _):
        for cp in dw_stores(e):
            cp.wait()
        return 0
    lax.fori_loop(0, n_loc, end_w, 0)


def dense_experts(h_all, dy_all, g_all, w_gate, w_up, w_down):
    n_blk, rows, d = h_all.shape
    n_loc, _, half = w_gate.shape
    flops = 18 * n_blk * rows * n_loc * d * half
    return pl.pallas_call(
        dense_kernel,
        out_shape=[jax.ShapeDtypeStruct((n_blk, rows, 2 * d), BF16),
                   jax.ShapeDtypeStruct((n_blk, rows, 128), F32),
                   jax.ShapeDtypeStruct(w_gate.shape, F32),
                   jax.ShapeDtypeStruct(w_up.shape, F32),
                   jax.ShapeDtypeStruct(w_down.shape, F32)],
        in_specs=[pl.BlockSpec(memory_space=pl.ANY)] * 6,
        out_specs=[pl.BlockSpec(memory_space=pl.ANY)] * 5,
        scratch_shapes=[
            pltpu.VMEM((2, rows, d), BF16), pltpu.VMEM((2, rows, d), BF16), pltpu.VMEM((2, rows, 128), F32),
            pltpu.VMEM((d, rows), BF16),
            pltpu.VMEM((n_loc, d, 2 * half), BF16), pltpu.VMEM((n_loc, half, d), BF16),
            pltpu.VMEM((n_loc, d, 2 * half), F32), pltpu.VMEM((n_loc, half, d), F32),
            pltpu.VMEM((rows, d), F32), pltpu.VMEM((rows, d), F32), pltpu.VMEM((rows, 128), F32),
            pltpu.VMEM((rows, 2 * d), BF16), pltpu.VMEM((rows, 128), F32),
            pltpu.SemaphoreType.DMA((2, 3)), pltpu.SemaphoreType.DMA((n_loc, 3)),
            pltpu.SemaphoreType.DMA((2,)), pltpu.SemaphoreType.DMA((n_loc, 3)),
        ],
        compiler_params=pltpu.CompilerParams(vmem_limit_bytes=66_000_000),
        cost_estimate=pl.CostEstimate(flops=flops, bytes_accessed=100_000_000, transcendentals=0),
        name="dense_experts",
    )(h_all, dy_all, g_all, w_gate, w_up, w_down)


def solution(mesh):
    tok_spec = P(("dp", "ep", "tp"), None)
    wide_spec = P("ep", None, "tp")
    down_spec = P("ep", "tp", None)
    grad_wide = P(("dp", "ep"), None, "tp")
    grad_down = P(("dp", "ep"), "tp", None)

    def device_step(x_in, norm_gain, w_router, expert_idx, w_gate, w_up, w_down, out_bias, dy_out):
        n_tok, d = x_in.shape
        n_exp = w_router.shape[1]
        n_loc = w_gate.shape[0]
        group = ("ep", "tp")
        x_f32 = x_in.astype(F32)
        inv_rms = lax.rsqrt(jnp.mean(x_f32 * x_f32, axis=-1, keepdims=True) + EPS)
        normed = x_f32 * inv_rms
        gain = norm_gain.astype(F32)
        hidden = (normed * gain).astype(BF16)
        logits = jnp.dot(hidden, w_router, preferred_element_type=F32)
        chosen = jnp.any(expert_idx[:, :, None] == jnp.arange(n_exp)[None, None, :], axis=1)
        gates = jax.nn.softmax(jnp.where(chosen, logits, -jnp.inf), axis=-1)
        h_all = lax.all_gather(hidden, group, axis=0)
        dy_all = lax.all_gather(dy_out, group, axis=0)
        g_all = lax.all_gather(gates, group, axis=0)
        my_ep = lax.axis_index("ep")
        g_loc = lax.dynamic_slice_in_dim(g_all, my_ep * n_loc, n_loc, axis=2)
        g_loc = jnp.pad(g_loc, ((0, 0), (0, 0), (0, 128 - n_loc)))
        tok, dg, d_gate, d_up, d_down = dense_experts(h_all, dy_all, g_loc, w_gate, w_up, w_down)
        tok = lax.psum_scatter(tok.reshape(-1, 2 * d), group, scatter_dimension=0, tiled=True)
        dg = lax.all_to_all(dg[:, :, :n_loc], group, 0, 0, tiled=True)
        dg = jnp.sum(dg.reshape(n_exp // n_loc, -1, n_tok, n_loc), axis=1)
        d_gates = jnp.transpose(dg, (1, 0, 2)).reshape(n_tok, n_exp)
        moe_out = tok[:, :d].astype(F32) + out_bias.astype(F32)
        y_out = (x_f32 + moe_out).astype(BF16)
        dy_f32 = dy_out.astype(F32)
        d_bias = jnp.sum(dy_f32, axis=0)
        d_logits = gates * (d_gates - jnp.sum(gates * d_gates, axis=-1, keepdims=True))
        d_router = jnp.einsum("td,te->de", hidden, d_logits, preferred_element_type=F32)
        dh_total = tok[:, d:].astype(F32) + jnp.einsum("te,de->td", d_logits, w_router, preferred_element_type=F32)
        d_gain = jnp.sum(dh_total * normed, axis=0)
        d_norm = dh_total * gain
        dx_in = (dy_f32 + inv_rms * (d_norm - normed * jnp.mean(d_norm * normed, axis=-1, keepdims=True))).astype(BF16)
        d_gain, d_router, d_bias = lax.psum((d_gain, d_router, d_bias), group)
        return y_out, dx_in, d_gain, d_router, d_gate, d_up, d_down, d_bias

    return jax.shard_map(device_step, mesh=mesh, in_specs=(tok_spec, P(None), P(None, None), tok_spec, wide_spec, wide_spec, down_spec, P(None), tok_spec), out_specs=(tok_spec, tok_spec, P("dp"), P("dp", None), grad_wide, grad_wide, grad_down, P("dp")), check_vma=False)
```

```python
import functools

import jax
import jax.numpy as jnp
from jax import lax
from jax.experimental import pallas as pl
from jax.experimental.pallas import tpu as pltpu
from jax.sharding import PartitionSpec as P

EPS = 1e-6
F32 = jnp.float32
BF16 = jnp.bfloat16


def dot_nn(a, b):
    return jnp.dot(a, b, preferred_element_type=F32)


def dot_nt(a, b):
    return lax.dot_general(a, b, (((1,), (1,)), ((), ())), preferred_element_type=F32)


def dot_tn(a, b):
    return lax.dot_general(a, b, (((0,), (0,)), ((), ())), preferred_element_type=F32)


def expert_step(e, first, h_ref, ht_ref, dy_ref, g_ref, wgu, wd, dwgu, dwd, out_acc, dh_acc, dg_acc):
    half = wd.shape[1]
    rows = h_ref.shape[0]
    lane = lax.broadcasted_iota(jnp.int32, (rows, 128), 1)
    gate = jnp.sum(jnp.where(lane == e, g_ref[...], 0.0), axis=1, keepdims=True)
    on = gate > 0.0
    au = dot_nn(h_ref[...], wgu[e])
    raw = dot_nt(dy_ref[...], wd[e])
    a = au[:, :half]
    u = au[:, half:]
    sig = jax.nn.sigmoid(a)
    silu = a * sig
    act = jnp.where(on, silu * u, 0.0).astype(BF16)
    dg = jnp.sum(jnp.where(on, act.astype(F32) * raw, 0.0), axis=1, keepdims=True)
    dg_acc[...] = jnp.where(lane == e, dg, dg_acc[...])
    d_act = gate * raw
    da = jnp.where(on, d_act * u * sig * (1.0 + a * (1.0 - sig)), 0.0).astype(BF16)
    du = jnp.where(on, d_act * silu, 0.0).astype(BF16)
    dau = jnp.concatenate([da, du], axis=1)
    out_acc[...] += gate * dot_nn(act, wd[e])
    dh_acc[...] += dot_nt(dau, wgu[e])
    dwgu[e] += dot_nn(ht_ref[...], dau)
    gdy = (gate * dy_ref[...].astype(F32)).astype(BF16)
    dwd[e] += dot_tn(act, gdy)


FLIPS = ((0, 0, 0), (0, 0, 1), (1, 0, 1), (0, 1, 0), (1, 1, 1), (1, 1, 0), (0, 1, 1), (1, 0, 0))
MIRROR = (0, 1, 6, 3, 4, 5, 2, 7)


def place(step):
    fa, fb, fc = FLIPS[step]
    ep = lax.axis_index("ep")
    y = lax.axis_index("tp")
    x = ep // 2
    c = ep % 2
    fx = fa * (1 - c) + fb * c
    fy = fa * c + fb * (1 - c)
    x2 = x + fx * (1 - 2 * x)
    y2 = y + fy * (1 - 2 * y)
    c2 = c + fc * (1 - 2 * c)
    return 2 * x2 + c2, y2


def dense_kernel(h_hbm, dy_hbm, gt_hbm, wg_hbm, wu_hbm, wd_hbm,
                 tok_own, tok_recv, dg_recv, h_buf, dy_buf, g_buf, dwg_hbm, dwu_hbm, dwd_hbm,
                 h_s, dy_s, gt_s, g_s, ht_s, wgu, wd, dwgu, dwd, out_acc, dh_acc, dg_acc, tok_s, dgt_s, pair_s,
                 in_sem, w_sem, dw_sem, ag_send, ag_recv, g_send, g_recv, tok_send, tok_rsem, pair_rsem, dg_send, dg_rsem, own_sem):
    rows, d = h_hbm.shape
    n_loc, _, half = wg_hbm.shape
    n_blk = len(FLIPS)
    my_ep = lax.axis_index("ep")
    my_blk = 2 * my_ep + lax.axis_index("tp")

    def remote(src, dst, send, recv, step):
        ep, tp = place(step)
        return pltpu.make_async_remote_copy(src_ref=src, dst_ref=dst, send_sem=send, recv_sem=recv,
                                            device_id={"ep": ep, "tp": tp}, device_id_type=pl.DeviceIdType.MESH)

    def rows_copy(i, src_step, dst_step, slot):
        hs = h_hbm if src_step == 0 else h_buf.at[src_step]
        ds = dy_hbm if src_step == 0 else dy_buf.at[src_step]
        return [remote(hs, h_buf.at[slot], ag_send.at[i, 0], ag_recv.at[slot, 0], dst_step),
                remote(ds, dy_buf.at[slot], ag_send.at[i, 1], ag_recv.at[slot, 1], dst_step)]

    own_to_partner = rows_copy(0, 0, 1, 1)
    own_to_b = rows_copy(1, 0, 3, 3)
    b_to_partner = rows_copy(2, 3, 1, 2)
    b_to_a = rows_copy(3, 3, 7, 5)
    own_to_a = rows_copy(4, 0, 7, 7)
    diag_to_partner = rows_copy(5, 5, 1, 4)
    a_to_partner = rows_copy(6, 7, 1, 6)

    def gate_copy(k):
        ep, _ = place(k)
        return remote(gt_hbm.at[pl.ds(pl.multiple_of(ep * n_loc, n_loc), n_loc), :], g_buf.at[MIRROR[k]], g_send.at[k], g_recv.at[MIRROR[k]], k)

    def dg_copy(k):
        return remote(dgt_s.at[k % 2], dg_recv.at[my_blk], dg_send.at[k], dg_rsem.at[MIRROR[k]], k)

    def tok_copy(k):
        src = tok_s.at[k % 2]
        if k % 2 == 0:
            i = (k - 2) // 2
            return remote(src, pair_s.at[i % 2], tok_send.at[k], pair_rsem.at[i], 1)
        i = (k - 1) // 2
        return remote(src, tok_recv.at[i], tok_send.at[k], tok_rsem.at[i], k)

    own_tok = pltpu.make_async_copy(tok_s.at[0], tok_own, own_sem.at[0])
    own_dg = pltpu.make_async_copy(dgt_s.at[0], dg_recv.at[my_blk], own_sem.at[1])

    def loads(c, slot):
        return [pltpu.make_async_copy(h_buf.at[c], h_s.at[slot], in_sem.at[slot, 0]),
                pltpu.make_async_copy(dy_buf.at[c], dy_s.at[slot], in_sem.at[slot, 1]),
                pltpu.make_async_copy(g_buf.at[c], gt_s.at[slot, pl.ds(0, n_loc), :], in_sem.at[slot, 2])]

    def own_loads():
        return [pltpu.make_async_copy(h_hbm, h_s.at[0], in_sem.at[0, 0]),
                pltpu.make_async_copy(dy_hbm, dy_s.at[0], in_sem.at[0, 1]),
                pltpu.make_async_copy(gt_hbm.at[pl.ds(pl.multiple_of(my_ep * n_loc, n_loc), n_loc), :],
                                      gt_s.at[0, pl.ds(0, n_loc), :], in_sem.at[0, 2])]

    def w_loads(e):
        return [pltpu.make_async_copy(wg_hbm.at[e], wgu.at[e, :, pl.ds(0, half)], w_sem.at[e, 0]),
                pltpu.make_async_copy(wu_hbm.at[e], wgu.at[e, :, pl.ds(half, half)], w_sem.at[e, 1]),
                pltpu.make_async_copy(wd_hbm.at[e], wd.at[e], w_sem.at[e, 2])]

    def dw_stores(e):
        return [pltpu.make_async_copy(dwgu.at[e, :, pl.ds(0, half)], dwg_hbm.at[e], dw_sem.at[e, 0]),
                pltpu.make_async_copy(dwgu.at[e, :, pl.ds(half, half)], dwu_hbm.at[e], dw_sem.at[e, 1]),
                pltpu.make_async_copy(dwd.at[e], dwd_hbm.at[e], dw_sem.at[e, 2])]

    def start(copies):
        for cp in copies:
            cp.start()

    def wait_recv(copies):
        for cp in copies:
            cp.wait_recv()

    gt_s[...] = jnp.zeros_like(gt_s)
    start(own_to_b)
    start(own_to_partner)
    start(own_loads())
    for k in range(1, n_blk):
        gate_copy(k).start()

    def start_w(e, _):
        start(w_loads(e))
        return 0
    lax.fori_loop(0, n_loc, start_w, 0)

    arrivals = {1: own_to_partner, 2: b_to_partner, 4: diag_to_partner, 6: a_to_partner}

    def block(s, _):
        slot = s % 2
        for cp in loads(s, slot):
            cp.wait()
        h_ref, dy_ref = h_s.at[slot], dy_s.at[slot]
        g_s[...] = gt_s[slot].T
        ht_s[...] = h_ref[...].T
        out_acc[...] = jnp.zeros_like(out_acc)
        dh_acc[...] = jnp.zeros_like(dh_acc)
        dg_acc[...] = jnp.zeros_like(dg_acc)

        def expert(e, _):
            @pl.when(s == 0)
            def _():
                for cp in w_loads(e):
                    cp.wait()
                dwgu[e] = jnp.zeros(dwgu.shape[1:], F32)
                dwd[e] = jnp.zeros(dwd.shape[1:], F32)

            @pl.when(jnp.logical_and(s == 1, e == 1))
            def _():
                wait_recv(own_to_b)
                start(b_to_partner)
                start(b_to_a)
                start(own_to_a)

            @pl.when(jnp.logical_and(s == 3, e == 0))
            def _():
                wait_recv(b_to_a)
                start(diag_to_partner)

            @pl.when(jnp.logical_and(s == 3, e == 4))
            def _():
                wait_recv(own_to_a)
                start(a_to_partner)

            for k in range(n_blk - 1):
                @pl.when(jnp.logical_and(s == k, e == n_loc - 1))
                def _():
                    if k + 1 in arrivals:
                        wait_recv(arrivals[k + 1])
                    gate_copy(MIRROR[k + 1]).wait_recv()
                    start(loads(k + 1, (k + 1) % 2))

            expert_step(e, None, h_ref, ht_s, dy_ref, g_s, wgu, wd, dwgu, dwd, out_acc, dh_acc, dg_acc)

            @pl.when(s == n_blk - 1)
            def _():
                start(dw_stores(e))
            return 0
        lax.fori_loop(0, n_loc, expert, 0)

        for k in range(2, n_blk):
            @pl.when(s == k)
            def _():
                if k == 2:
                    own_tok.wait()
                    own_dg.wait()
                else:
                    tok_copy(k - 2).wait_send()
                    dg_copy(k - 2).wait_send()
        tile = rows // 8
        is_pair = jnp.logical_and(s % 2 == 1, s > 1)

        @pl.when(is_pair)
        def _():
            for k in (3, 5, 7):
                @pl.when(s == k)
                def _():
                    tok_copy(k - 1).wait_recv()
            side = ((s - 3) // 2) % 2

            def fold(i, _):
                r = pl.ds(pl.multiple_of(i * tile, tile), tile)
                tok_s[slot, r, pl.ds(0, d)] = (out_acc[r, :] + pair_s[side, r, pl.ds(0, d)].astype(F32)).astype(BF16)
                tok_s[slot, r, pl.ds(d, d)] = (dh_acc[r, :] + pair_s[side, r, pl.ds(d, d)].astype(F32)).astype(BF16)
                return 0
            lax.fori_loop(0, 8, fold, 0)

        @pl.when(jnp.logical_not(is_pair))
        def _():
            def keep(i, _):
                r = pl.ds(pl.multiple_of(i * tile, tile), tile)
                tok_s[slot, r, pl.ds(0, d)] = out_acc[r, :].astype(BF16)
                tok_s[slot, r, pl.ds(d, d)] = dh_acc[r, :].astype(BF16)
                return 0
            lax.fori_loop(0, 8, keep, 0)
        dgt_s[slot] = dg_acc[...].T[:n_loc]
        for k in range(n_blk):
            @pl.when(s == k)
            def _():
                if k == 0:
                    own_tok.start()
                    own_dg.start()
                else:
                    tok_copy(k).start()
                    dg_copy(k).start()
        return 0

    lax.fori_loop(0, n_blk, block, 0)

    for k in (6, 7):
        tok_copy(k).wait_send()
        dg_copy(k).wait_send()
    for k in (1, 3, 5, 7):
        tok_copy(k).wait_recv()
    for k in range(1, n_blk):
        dg_copy(MIRROR[k]).wait_recv()
        gate_copy(k).wait_send()
    for copies in (own_to_partner, own_to_b, b_to_partner, b_to_a, own_to_a, diag_to_partner, a_to_partner):
        for cp in copies:
            cp.wait_send()

    def end_w(e, _):
        for cp in dw_stores(e):
            cp.wait()
        return 0
    lax.fori_loop(0, n_loc, end_w, 0)


def dense_experts(hidden, dy, gates_t, w_gate, w_up, w_down):
    rows, d = hidden.shape
    n_loc, _, half = w_gate.shape
    n_blk = len(FLIPS)
    flops = 18 * n_blk * rows * n_loc * d * half
    dma = pltpu.SemaphoreType.DMA
    out = pl.pallas_call(
        dense_kernel,
        out_shape=[jax.ShapeDtypeStruct((rows, 2 * d), BF16),
                   jax.ShapeDtypeStruct((4, rows, 2 * d), BF16),
                   jax.ShapeDtypeStruct((n_blk, n_loc, rows), F32),
                   jax.ShapeDtypeStruct((n_blk, rows, d), BF16),
                   jax.ShapeDtypeStruct((n_blk, rows, d), BF16),
                   jax.ShapeDtypeStruct((n_blk, n_loc, rows), F32),
                   jax.ShapeDtypeStruct(w_gate.shape, F32),
                   jax.ShapeDtypeStruct(w_up.shape, F32),
                   jax.ShapeDtypeStruct(w_down.shape, F32)],
        in_specs=[pl.BlockSpec(memory_space=pl.ANY)] * 6,
        out_specs=[pl.BlockSpec(memory_space=pl.ANY)] * 9,
        scratch_shapes=[
            pltpu.VMEM((2, rows, d), BF16), pltpu.VMEM((2, rows, d), BF16),
            pltpu.VMEM((2, 128, rows), F32), pltpu.VMEM((rows, 128), F32),
            pltpu.VMEM((d, rows), BF16),
            pltpu.VMEM((n_loc, d, 2 * half), BF16), pltpu.VMEM((n_loc, half, d), BF16),
            pltpu.VMEM((n_loc, d, 2 * half), F32), pltpu.VMEM((n_loc, half, d), F32),
            pltpu.VMEM((rows, d), F32), pltpu.VMEM((rows, d), F32), pltpu.VMEM((rows, 128), F32),
            pltpu.VMEM((2, rows, 2 * d), BF16), pltpu.VMEM((2, n_loc, rows), F32),
            pltpu.VMEM((2, rows, 2 * d), BF16),
            dma((2, 3)), dma((n_loc, 3)), dma((n_loc, 3)),
            dma((7, 2)), dma((n_blk, 2)), dma((n_blk,)), dma((n_blk,)),
            dma((n_blk,)), dma((4,)), dma((3,)), dma((n_blk,)), dma((n_blk,)), dma((2,)),
        ],
        compiler_params=pltpu.CompilerParams(vmem_limit_bytes=67_000_000, has_side_effects=True),
        cost_estimate=pl.CostEstimate(flops=flops, bytes_accessed=100_000_000, transcendentals=0),
        name="dense_experts",
    )(hidden, dy, gates_t, w_gate, w_up, w_down)
    return out[0], out[1], out[2], out[6], out[7], out[8]


def solution(mesh):
    tok_spec = P(("dp", "ep", "tp"), None)
    wide_spec = P("ep", None, "tp")
    down_spec = P("ep", "tp", None)
    grad_wide = P(("dp", "ep"), None, "tp")
    grad_down = P(("dp", "ep"), "tp", None)

    def device_step(x_in, norm_gain, w_router, expert_idx, w_gate, w_up, w_down, out_bias, dy_out):
        n_tok, d = x_in.shape
        n_exp = w_router.shape[1]
        n_loc = w_gate.shape[0]
        group = ("ep", "tp")
        x_f32 = x_in.astype(F32)
        inv_rms = lax.rsqrt(jnp.mean(x_f32 * x_f32, axis=-1, keepdims=True) + EPS)
        normed = x_f32 * inv_rms
        gain = norm_gain.astype(F32)
        hidden = (normed * gain).astype(BF16)
        logits = jnp.dot(hidden, w_router, preferred_element_type=F32)
        chosen = jnp.any(expert_idx[:, :, None] == jnp.arange(n_exp)[None, None, :], axis=1)
        gates = jax.nn.softmax(jnp.where(chosen, logits, -jnp.inf), axis=-1)
        tok_own, tok_recv, dg, d_gate, d_up, d_down = dense_experts(hidden, dy_out, gates.T, w_gate, w_up, w_down)
        tok = tok_own.astype(F32) + jnp.sum(tok_recv.astype(F32), axis=0)
        d_gates = jnp.sum(dg.reshape(-1, 2, n_loc, n_tok), axis=1).reshape(n_exp, n_tok).T
        moe_out = tok[:, :d] + out_bias.astype(F32)
        y_out = (x_f32 + moe_out).astype(BF16)
        dy_f32 = dy_out.astype(F32)
        d_bias = jnp.sum(dy_f32, axis=0)
        d_logits = gates * (d_gates - jnp.sum(gates * d_gates, axis=-1, keepdims=True))
        d_router = jnp.einsum("td,te->de", hidden, d_logits, preferred_element_type=F32)
        dh_total = tok[:, d:] + jnp.einsum("te,de->td", d_logits, w_router, preferred_element_type=F32)
        d_gain = jnp.sum(dh_total * normed, axis=0)
        d_norm = dh_total * gain
        dx_in = (dy_f32 + inv_rms * (d_norm - normed * jnp.mean(d_norm * normed, axis=-1, keepdims=True))).astype(BF16)
        sums = lax.psum(jnp.concatenate([d_router.T, d_gain[None], d_bias[None]], axis=0), group)
        d_router, d_gain, d_bias = sums[:n_exp].T, sums[n_exp], sums[n_exp + 1]
        return y_out, dx_in, d_gain, d_router, d_gate, d_up, d_down, d_bias

    return jax.shard_map(device_step, mesh=mesh, in_specs=(tok_spec, P(None), P(None, None), tok_spec, wide_spec, wide_spec, down_spec, P(None), tok_spec), out_specs=(tok_spec, tok_spec, P("dp"), P("dp", None), grad_wide, grad_wide, grad_down, P("dp")), check_vma=False)
```
